32 devices in a mesh: part: 2 (over x), loc: 4 (over z), grp: 4 (over y, core).
Axes of the slice: x: 2, y: 2, z: 4, core: 2. Of those that a mesh axis runs over, the one named last changes fastest.
Arguments:
- x_rows: bfloat16 [49152, 512], P(('part', 'grp', 'loc')), parts along dimension 0
- dy_rows: bfloat16 [49152, 512], P(('part', 'grp', 'loc')), parts along dimension 0
- expert_ids: int32 [49152, 4], P(('part', 'grp', 'loc')), parts along dimension 0
- gate_vals: float32 [49152, 4], P(('part', 'grp', 'loc')), parts along dimension 0
- w_gate: bfloat16 [32, 512, 896], P(('part', 'grp', 'loc')), parts along dimension 0
- w_up: bfloat16 [32, 512, 896], P(('part', 'grp', 'loc')), parts along dimension 0
- w_down: bfloat16 [32, 896, 512], P(('part', 'grp', 'loc')), parts along dimension 0
Outputs:
- output 1: bfloat16 [49152, 512], P(('part', 'grp', 'loc')), parts along dimension 0
- output 2: float32 [49152, 4], P(('part', 'grp', 'loc')), parts along dimension 0
- output 3: bfloat16 [32, 512, 896], P(('part', 'grp', 'loc')), parts along dimension 0
- output 4: bfloat16 [32, 512, 896], P(('part', 'grp', 'loc')), parts along dimension 0
- output 5: bfloat16 [32, 896, 512], P(('part', 'grp', 'loc')), parts along dimension 0
There are 2 independent parts. The reference program is written for one: setup_inputs(seed, part) draws one part's arguments, and reference() takes and returns one part's arrays. A program takes and returns all parts, laid end to end along the dimension named above; each array names one.
All inputs are finite; a program needn't handle non-finite values.
Results may differ from the reference program's by a relative error of at most 0.001.
Values are sent between devices in bfloat16 or wider.
A program may use at most 1 GiB of HBM per device.

```python
import jax
import jax.numpy as jnp
from jax import lax

GROUPS = 4
LOC_DEVS = 4
TOK_DEV = 1536
EXPERTS = 16
TOP_K = 4
D_MODEL = 512
D_FF = 896

DEV_COUNT = GROUPS * LOC_DEVS
TOKENS = TOK_DEV * DEV_COUNT
NUM_ITEMS = TOKENS * TOP_K
GROUP_LIMIT = min(TOP_K // 2, GROUPS)
PER_GROUP = TOP_K // GROUP_LIMIT
GROUP_EXPERTS = EXPERTS // GROUPS
GROUP_ROWS = GROUP_LIMIT * TOK_DEV // GROUPS
MEAN_LOAD = TOK_DEV * TOP_K // EXPERTS
SPREAD_MAX = min(MEAN_LOAD, GROUP_ROWS - MEAN_LOAD)
EXPERT_CAP = DEV_COUNT * (MEAN_LOAD + SPREAD_MAX)


def block_routing(block_key):
    key_sig, key_off, key_perm, key_amp, key_slot = jax.random.split(block_key, 5)
    tok_perm = jax.random.permutation(key_sig, TOK_DEV)
    offsets = jax.random.permutation(key_off, GROUPS)[:GROUP_LIMIT]
    shifted = (tok_perm[:, None] + offsets[None, :]) % TOK_DEV
    group_of = shifted % GROUPS
    pair_pos = jnp.arange(GROUP_LIMIT)[None, :] * (TOK_DEV // GROUPS) + shifted // GROUPS
    local_perm = jax.vmap(lambda sub_key: jax.random.permutation(sub_key, GROUP_EXPERTS))(jax.random.split(key_perm, GROUPS))
    spread = jax.random.randint(key_amp, (GROUPS, GROUP_EXPERTS // 2), 0, SPREAD_MAX + 1)
    spread = spread.at[:, 0].set(SPREAD_MAX)
    counts = jnp.stack([MEAN_LOAD + spread, MEAN_LOAD - spread], axis=-1).reshape(GROUPS, GROUP_EXPERTS)
    cum_ends = jnp.cumsum(counts, axis=1)
    seq_pos = jnp.arange(PER_GROUP)[None, None, :] * GROUP_ROWS + pair_pos[:, :, None]
    rank_idx = jnp.sum(seq_pos[..., None] >= cum_ends[group_of][:, :, None, :], axis=-1)
    local_ids = local_perm[group_of[:, :, None], rank_idx]
    expert = (group_of[:, :, None] * GROUP_EXPERTS + local_ids).reshape(TOK_DEV, TOP_K)
    slot_keys = jax.random.randint(key_slot, (TOK_DEV, TOP_K), 0, 4096) * TOP_K + jnp.arange(TOP_K)[None, :]
    slot_order = jnp.argsort(slot_keys, axis=1)
    return jnp.take_along_axis(expert, slot_order, axis=1).astype(jnp.int32)


def draw_routing(route_key):
    blocks = jax.vmap(block_routing)(jax.random.split(route_key, DEV_COUNT))
    return blocks.reshape(TOKENS, TOP_K)


def setup_inputs(seed: int = 0, part: int = 0) -> dict:
    base_key = jax.random.fold_in(jax.random.key(seed), part)
    keys = jax.random.split(base_key, 7)
    x_rows = jax.random.normal(keys[0], (TOKENS, D_MODEL), jnp.float32).astype(jnp.bfloat16)
    dy_rows = jax.random.normal(keys[1], (TOKENS, D_MODEL), jnp.float32).astype(jnp.bfloat16)
    expert_ids = draw_routing(keys[2])
    gate_vals = jax.random.uniform(keys[3], (TOKENS, TOP_K), jnp.float32, 0.25, 1.0)
    w_gate = (jax.random.normal(keys[4], (EXPERTS, D_MODEL, D_FF), jnp.float32) * D_MODEL ** -0.5).astype(jnp.bfloat16)
    w_up = (jax.random.normal(keys[5], (EXPERTS, D_MODEL, D_FF), jnp.float32) * D_MODEL ** -0.5).astype(jnp.bfloat16)
    w_down = (jax.random.normal(keys[6], (EXPERTS, D_FF, D_MODEL), jnp.float32) * D_FF ** -0.5).astype(jnp.bfloat16)
    return {'x_rows': x_rows, 'dy_rows': dy_rows, 'expert_ids': expert_ids, 'gate_vals': gate_vals, 'w_gate': w_gate, 'w_up': w_up, 'w_down': w_down}


def expert_lists(expert_ids):
    flat_ids = expert_ids.reshape(-1)
    item_order = jnp.argsort(flat_ids, stable=True)
    sorted_ids = flat_ids[item_order]
    load_sizes = jnp.zeros((EXPERTS,), jnp.int32).at[flat_ids].add(1)
    starts = jnp.cumsum(load_sizes) - load_sizes
    slot_rank = jnp.arange(NUM_ITEMS) - starts[sorted_ids]
    slot_lists = jnp.full((EXPERTS * EXPERT_CAP,), NUM_ITEMS, jnp.int32)
    slot_lists = slot_lists.at[sorted_ids * EXPERT_CAP + slot_rank].set(item_order.astype(jnp.int32))
    return slot_lists.reshape(GROUPS, GROUP_EXPERTS, EXPERT_CAP)


def reference(x_rows, dy_rows, expert_ids, gate_vals, w_gate, w_up, w_down):
    slot_lists = expert_lists(expert_ids)
    gate_flat = gate_vals.reshape(-1)

    def expert_step(part_sum, inputs):
        slot_items, wg_one, wu_one, wd_one = inputs
        is_live = slot_items < NUM_ITEMS
        tok_idx = jnp.where(is_live, slot_items // TOP_K, 0)
        x_sel = jnp.where(is_live[:, None], x_rows[tok_idx], 0).astype(jnp.bfloat16)
        dy_sel = jnp.where(is_live[:, None], dy_rows[tok_idx], 0).astype(jnp.bfloat16)
        gate_sel = jnp.where(is_live, gate_flat[jnp.minimum(slot_items, NUM_ITEMS - 1)], 0.0)
        pre_gate = jnp.dot(x_sel, wg_one, preferred_element_type=jnp.float32)
        pre_up = jnp.dot(x_sel, wu_one, preferred_element_type=jnp.float32)
        sig_gate = jax.nn.sigmoid(pre_gate)
        silu_out = pre_gate * sig_gate
        hidden = (silu_out * pre_up).astype(jnp.bfloat16)
        expert_out = jnp.dot(hidden, wd_one, preferred_element_type=jnp.float32)
        dgate_sel = jnp.sum(dy_sel.astype(jnp.float32) * expert_out, axis=-1)
        d_out = (gate_sel[:, None] * dy_sel.astype(jnp.float32)).astype(jnp.bfloat16)
        d_hidden = jnp.dot(d_out, wd_one.T, preferred_element_type=jnp.float32)
        dwd_one = jnp.dot(hidden.T, d_out, preferred_element_type=jnp.float32).astype(jnp.bfloat16)
        d_pre_up = (d_hidden * silu_out).astype(jnp.bfloat16)
        d_pre_gate = (d_hidden * pre_up * sig_gate * (1.0 + pre_gate * (1.0 - sig_gate))).astype(jnp.bfloat16)
        dwg_one = jnp.dot(x_sel.T, d_pre_gate, preferred_element_type=jnp.float32).astype(jnp.bfloat16)
        dwu_one = jnp.dot(x_sel.T, d_pre_up, preferred_element_type=jnp.float32).astype(jnp.bfloat16)
        d_rows = (jnp.dot(d_pre_gate, wg_one.T, preferred_element_type=jnp.float32) + jnp.dot(d_pre_up, wu_one.T, preferred_element_type=jnp.float32)).astype(jnp.bfloat16)
        part_sum = part_sum.at[tok_idx].add(d_rows.astype(jnp.float32))
        return part_sum, (dwg_one, dwu_one, dwd_one, dgate_sel)

    def group_step(dx_acc, inputs):
        part_sum, outputs = lax.scan(expert_step, jnp.zeros((TOKENS, D_MODEL), jnp.float32), inputs)
        return dx_acc + part_sum.astype(jnp.bfloat16).astype(jnp.float32), outputs

    weights = (w_gate.reshape(GROUPS, GROUP_EXPERTS, D_MODEL, D_FF), w_up.reshape(GROUPS, GROUP_EXPERTS, D_MODEL, D_FF), w_down.reshape(GROUPS, GROUP_EXPERTS, D_FF, D_MODEL))
    dx_acc, outputs = lax.scan(group_step, jnp.zeros((TOKENS, D_MODEL), jnp.float32), (slot_lists,) + weights)
    dw_gate, dw_up, dw_down, dgate_vals = outputs
    d_gates = jnp.zeros((NUM_ITEMS + 1,), jnp.float32).at[slot_lists.reshape(-1)].set(dgate_vals.reshape(-1))
    return (dx_acc.astype(jnp.bfloat16), d_gates[:NUM_ITEMS].reshape(TOKENS, TOP_K), dw_gate.reshape(EXPERTS, D_MODEL, D_FF), dw_up.reshape(EXPERTS, D_MODEL, D_FF), dw_down.reshape(EXPERTS, D_FF, D_MODEL))
```

```python
import functools

import jax
import jax.numpy as jnp
from jax import lax
from jax.experimental import pallas as pl
from jax.experimental.pallas import tpu as pltpu
from jax.sharding import PartitionSpec as P

BF = jnp.bfloat16
F32 = jnp.float32
NT = (((1,), (1,)), ((), ()))
TN = (((0,), (0,)), ((), ()))


def expert_kernel(n_tiles, first, valid_ref, blk_ref, meta_ref, wg_ref, wu_ref, wd_ref, *rest):
    if first:
        c_ref, d_ref, acc_ref, xs_ref, us_ref, h_ref, da_ref, db_ref = rest
    else:
        old_ref, c_ref, d_ref, acc_ref, xs_ref, us_ref, h_ref, da_ref, db_ref = rest
    step = pl.program_id(0)
    half = blk_ref.shape[0] // 2
    d_model = blk_ref.shape[1] // 2
    rows = half // n_tiles

    @pl.when(valid_ref[0] == 1)
    def _():
        for tile in range(n_tiles):
            lo = tile * rows
            at = pl.ds(lo, rows)
            gate = meta_ref[at, 0:1]
            code = meta_ref[at, 1:2]
            in_a = code == 1.0
            in_b = code == 2.0

            def pick(col):
                top = blk_ref[pl.ds(lo, rows), pl.ds(col, d_model)].astype(F32)
                low = blk_ref[pl.ds(half + lo, rows), pl.ds(col, d_model)].astype(F32)
                return jnp.where(in_a, top, jnp.where(in_b, low, 0.0))

            x = pick(0).astype(BF)
            dy = pick(d_model)
            u = (gate * dy).astype(BF)
            xs_ref[at, :] = x
            us_ref[at, :] = u
            a = jnp.dot(x, wg_ref[...], preferred_element_type=F32)
            b = jnp.dot(x, wu_ref[...], preferred_element_type=F32)
            sig = jax.nn.sigmoid(a)
            silu = a * sig
            h = (silu * b).astype(BF)
            h_ref[at, :] = h
            o = jnp.dot(h, wd_ref[...], preferred_element_type=F32)
            d_ref[at, :] = jnp.sum(dy * o, axis=1, keepdims=True)
            dh = lax.dot_general(u, wd_ref[...], NT, preferred_element_type=F32)
            db = (dh * silu).astype(BF)
            da = (dh * b * sig * (1.0 + a * (1.0 - sig))).astype(BF)
            da_ref[at, :] = da
            db_ref[at, :] = db
            c = lax.dot_general(da, wg_ref[...], NT, preferred_element_type=F32)
            c = c + lax.dot_general(db, wu_ref[...], NT, preferred_element_type=F32)
            c_ref[at, :] = c.astype(BF)
        terms = ((xs_ref, da_ref), (xs_ref, db_ref), (us_ref, h_ref))
        for k, (left, right) in enumerate(terms):
            part = lax.dot_general(left[...], right[...], TN, preferred_element_type=F32)
            acc_ref[k] = part if first else old_ref[k] + part

    if not first:
        @pl.when(jnp.logical_and(valid_ref[0] == 0, step == 0))
        def _():
            acc_ref[...] = old_ref[...]


def expert_call(blk, meta, wg, wu, wd, acc, valid):
    n_grp, d_model, d_ff = wg.shape
    half = blk.shape[0] // 2
    first = acc is None
    pick = lambda g, v: (g * v[0], 0, 0)
    pick4 = lambda g, v: (g * v[0], 0, 0, 0)
    acc_spec = pl.BlockSpec((None, 3, d_model, d_ff), pick4)
    in_specs = [
        pl.BlockSpec((2 * half, 2 * d_model), lambda g, v: (0, 0)),
        pl.BlockSpec((None, half, 2), pick),
        pl.BlockSpec((None, d_model, d_ff), pick),
        pl.BlockSpec((None, d_model, d_ff), pick),
        pl.BlockSpec((None, d_ff, d_model), pick),
    ]
    args = [valid, blk, meta, wg, wu, wd]
    aliases = {}
    if not first:
        in_specs.append(acc_spec)
        args.append(acc)
        aliases = {6: 2}
    return pl.pallas_call(
        functools.partial(expert_kernel, 3, first),
        grid_spec=pltpu.PrefetchScalarGridSpec(
            num_scalar_prefetch=1,
            grid=(n_grp,),
            in_specs=in_specs,
            out_specs=[
                pl.BlockSpec((None, half, d_model), pick),
                pl.BlockSpec((None, half, 1), pick),
                acc_spec,
            ],
            scratch_shapes=[
                pltpu.VMEM((half, d_model), BF),
                pltpu.VMEM((half, d_model), BF),
                pltpu.VMEM((half, d_ff), BF),
                pltpu.VMEM((half, d_ff), BF),
                pltpu.VMEM((half, d_ff), BF),
            ],
        ),
        out_shape=[
            jax.ShapeDtypeStruct((n_grp, half, d_model), BF),
            jax.ShapeDtypeStruct((n_grp, half, 1), F32),
            jax.ShapeDtypeStruct((n_grp, 3, d_model, d_ff), F32),
        ],
        input_output_aliases=aliases,
        cost_estimate=pl.CostEstimate(
            flops=18 * n_grp * half * d_model * d_ff, bytes_accessed=70_000_000, transcendentals=0),
        compiler_params=pltpu.CompilerParams(dimension_semantics=('arbitrary',), vmem_limit_bytes=63_000_000),
    )(*args)


def add_bf(*terms):
    total = terms[0].astype(F32)
    for term in terms[1:]:
        total = total + term.astype(F32)
    return total.astype(BF)


def solution(mesh):
    grp_size = mesh.shape['grp']
    loc_size = mesh.shape['loc']
    spec = P(('part', 'grp', 'loc'))

    def device_step(x_rows, dy_rows, expert_ids, gate_vals, w_gate, w_up, w_down):
        n_tok, d_model = x_rows.shape
        half = n_tok // 2
        n_exp = grp_size * loc_size
        loc = lax.axis_index('loc')

        groups = expert_ids // loc_size
        in_group = [jnp.any(groups == g, axis=1) for g in range(grp_size)]
        in_a = in_group[0]
        classes = [in_a & in_group[m] for m in (1, 2, 3)]
        classes += [jnp.logical_not(in_a) & jnp.logical_not(in_group[m]) for m in (1, 2, 3)]
        onehot = jnp.stack(classes, axis=1)
        tok = jnp.arange(n_tok, dtype=jnp.int32)
        earlier = (tok[None, :] < tok[:, None]).astype(BF)
        rank = jnp.dot(earlier, onehot.astype(BF), preferred_element_type=F32)
        sizes = jnp.sum(onehot.astype(F32), axis=0)
        off = jnp.cumsum(sizes) - sizes
        pos = jnp.sum(jnp.where(onehot, rank + off[None, :], 0.0), axis=1).astype(jnp.int32)
        to_pos = (tok[:, None] == pos[None, :]).astype(BF)
        blk = jnp.dot(to_pos, jnp.concatenate([x_rows, dy_rows], axis=1), preferred_element_type=F32).astype(BF)

        exp_iota = jnp.arange(n_exp, dtype=jnp.int32)
        hit = expert_ids[:, :, None] == exp_iota[None, None, :]
        gate_tok = jnp.sum(jnp.where(hit, gate_vals[:, :, None], 0.0), axis=1)
        hit_tok = jnp.any(hit, axis=1).astype(F32)
        tok_meta = jnp.concatenate([gate_tok, hit_tok], axis=1)
        pos_meta = jnp.dot(to_pos.astype(F32), tok_meta, precision=lax.Precision.HIGHEST, preferred_element_type=F32)
        gate_pos = pos_meta[:half, :n_exp] + pos_meta[half:, :n_exp]
        code_pos = pos_meta[:half, n_exp:] + 2.0 * pos_meta[half:, n_exp:]
        meta = jnp.concatenate([gate_pos.T, code_pos.T], axis=0)
        meta_all = lax.all_gather(meta, 'loc', axis=0).reshape(loc_size, 2, grp_size, loc_size, half)
        meta_mine = lax.dynamic_index_in_dim(meta_all, loc, axis=3, keepdims=False)
        meta_mine = jnp.transpose(meta_mine, (0, 2, 3, 1))

        wg = lax.all_gather(w_gate, 'grp', axis=0, tiled=True)
        wu = lax.all_gather(w_up, 'grp', axis=0, tiled=True)
        wd = lax.all_gather(w_down, 'grp', axis=0, tiled=True)

        right_of, left_of = [], []
        hop_r, hop_l = blk, blk
        for k in range(1, loc_size):
            hop_r = lax.ppermute(hop_r, 'loc', [(i, i + 1) for i in range(k - 1, loc_size - 1)])
            hop_l = lax.ppermute(hop_l, 'loc', [(i, i - 1) for i in range(1, loc_size - k + 1)])
            right_of.append(hop_r)
            left_of.append(hop_l)

        def run(block, src, ok, acc):
            meta_src = lax.dynamic_index_in_dim(meta_mine, jnp.clip(src, 0, loc_size - 1), axis=0, keepdims=False)
            return expert_call(block, meta_src, wg, wu, wd, acc, ok.astype(jnp.int32).reshape(1))

        c_own, d_own, acc = run(blk, loc, loc >= 0, None)
        c_right, c_left, d_right, d_left = [], [], [], []
        for k in range(1, loc_size):
            c, d, acc = run(right_of[k - 1], loc - k, loc >= k, acc)
            c_right.append(c)
            d_right.append(d)
            c, d, acc = run(left_of[k - 1], loc + k, loc + k < loc_size, acc)
            c_left.append(c)
            d_left.append(d)

        back_l, back_r = None, None
        for k in range(loc_size - 1, 0, -1):
            send = c_right[k - 1] if back_l is None else add_bf(c_right[k - 1], back_l)
            back_l = lax.ppermute(send, 'loc', [(i, i - 1) for i in range(k, loc_size)])
            send = c_left[k - 1] if back_r is None else add_bf(c_left[k - 1], back_r)
            back_r = lax.ppermute(send, 'loc', [(i, i + 1) for i in range(0, loc_size - k)])

        dw = lax.psum_scatter(acc, 'grp', scatter_dimension=0, tiled=True).astype(BF)
        dw_gate = dw[:, 0]
        dw_up = dw[:, 1]
        dw_down = jnp.swapaxes(dw[:, 2], 1, 2)

        code_own = meta[n_exp:].reshape(grp_size, loc_size, half)
        grp_a = jnp.any(code_own == 1.0, axis=1)
        total = c_own.astype(F32) + back_l.astype(F32) + back_r.astype(F32)
        total = lax.reduce_precision(total, exponent_bits=8, mantissa_bits=7)
        dx_a = jnp.sum(jnp.where(grp_a[:, :, None], total, 0.0), axis=0)
        dx_b = jnp.sum(jnp.where(grp_a[:, :, None], 0.0, total), axis=0)
        dx_pos = jnp.concatenate([dx_a, dx_b], axis=0).astype(BF)
        from_pos = (pos[:, None] == tok[None, :]).astype(BF)
        dx = jnp.dot(from_pos, dx_pos, preferred_element_type=F32).astype(BF)

        d_slots = jnp.stack([d_own] + d_right + d_left)[..., 0]
        d_all = lax.all_gather(d_slots, 'loc', axis=0)
        per_loc = []
        for dev in range(loc_size):
            delta = dev - loc
            slot = jnp.where(delta >= 0, delta, loc_size - 1 - delta)
            per_loc.append(lax.dynamic_index_in_dim(d_all[dev], slot, axis=0, keepdims=False))
        d_exp = jnp.stack(per_loc, axis=1)
        d_exp = d_exp.reshape(n_exp, half)
        code_exp = meta[n_exp:]
        d_a = jnp.where(code_exp == 1.0, d_exp, 0.0)
        d_b = jnp.where(code_exp == 2.0, d_exp, 0.0)
        d_pos = jnp.concatenate([d_a, d_b], axis=1)
        d_tok = lax.dot_general(from_pos.astype(F32), d_pos, NT, precision=lax.Precision.HIGHEST, preferred_element_type=F32)
        d_gates = jnp.sum(jnp.where(hit, d_tok[:, None, :], 0.0), axis=2)
        return dx, d_gates, dw_gate, dw_up, dw_down

    return jax.shard_map(device_step, mesh=mesh, in_specs=(spec,) * 7, out_specs=(spec,) * 5, check_vma=False)
```
